128 devices in a mesh: node: 8 (over x, core), local: 16 (over y, z).
Axes of the slice: x: 4, y: 4, z: 4, core: 2. Of those that a mesh axis runs over, the one named last changes fastest.
Arguments:
- tokens: bfloat16 [2048, 7168], P('node', 'local'), may hold values from -6 to 6
- grad_out: bfloat16 [2048, 7168], P('node', 'local'), may hold values from -0.59765625 to 0.59765625
- gates: bfloat16 [2048, 8], P('node'), may hold values from 0.05 to 10
- routes: int32 [2048, 8], P('node'), may hold values from 0 to 31, all different within a row; in each aligned block of 256 rows (0 to 255, 256 to 511, ...) at most 80 rows name the same one
- w_gate: bfloat16 [32, 7168, 1024], P('node', 'local'), may hold values from -0.09375 to 0.09375
- w_up: bfloat16 [32, 7168, 1024], P('node', 'local'), may hold values from -0.09375 to 0.09375
- w_down: bfloat16 [32, 1024, 7168], P('node', None, 'local'), may hold values from -0.25 to 0.25
Outputs:
- grad_tokens: bfloat16 [2048, 7168], P('node', 'local')
- grad_gates: bfloat16 [2048, 8], P('node')
- grad_w_gate: bfloat16 [32, 7168, 1024], P('node', 'local')
- grad_w_up: bfloat16 [32, 7168, 1024], P('node', 'local')
- grad_w_down: bfloat16 [32, 1024, 7168], P('node', None, 'local')
- loads: float32 [32], replicated
The draws below stay inside these ranges and needn't reach their ends.
Inputs may be any that keep to these rules, and one draw needn't show every extreme that they name: `routes`: each row names 8 different experts. Within each aligned block of 256 rows (the rows of one index of node) no expert is named by more than 80 rows, and in some blocks one expert is named by exactly 80 rows.
All inputs are finite; a program needn't handle non-finite values.
Results may differ from the reference program's by a relative error of at most 0.033.
Values may be sent and summed in bfloat16 or wider, within the bound.
No kernel may reach another device: no remote copies, remote signals or barrier semaphores. Data moves between devices by JAX's collectives and lax.ppermute only.
A program may use at most 128 MiB of HBM per device.

```python
import math
import jax
import jax.numpy as jnp
import numpy as np
from jax import lax

D = 7168
H = 1024
TOP = 8
TOK_NODE = 256
EXPERTS = 32
CAP = 80
TOKENS = 2048
N_NODE = 8
N_LOCAL = 16


def draw_gates(key, part):
    block_count = TOKENS // TOK_NODE
    block_ids = (jnp.arange(TOKENS, dtype=jnp.int32) // TOK_NODE).astype(jnp.float32)
    frac = block_ids / max(block_count - 1, 1)
    logs = jax.random.uniform(key, (TOKENS, TOP), jnp.float32, jnp.log(0.05), 0.0)
    base = jnp.exp(logs)
    scale = jnp.exp(frac * jnp.log(10.0))
    values = jnp.clip(base * scale[:, None], 0.05, 10.0)
    return values.astype(jnp.bfloat16)


def strengthened(values, rng, source, target, shards_of, factor):
    def block_of(dim):
        return (jnp.arange(values.shape[dim]) // (values.shape[dim] // shards_of)).reshape((-1,) + (1,) * (values.ndim - 1 - dim))

    first = jax.random.permutation(rng, shards_of)[block_of(target)]
    second = (block_of(target) + shards_of // 2) % shards_of
    return jnp.where((block_of(source) == first) | (block_of(source) == second), factor * values, values)


def block_scale(own_key, dims, cuts, smallest, high):
    level, own = 1.0, jax.random.fold_in(own_key, 6)
    for dim, shards_of in cuts:
        draws = jnp.exp(jax.random.uniform(jax.random.fold_in(own, dim), (shards_of,), jnp.float32, smallest / len(cuts), high / len(cuts)))
        level = level * jnp.repeat(draws, dims[dim] // shards_of).reshape([-1 if axis == dim else 1 for axis in range(len(dims))])
    return level


def deal_out(stream_key, own, number, rows, amount, top, most, slope):
    order = jax.random.permutation(stream_key, amount)
    crowded, usual = portions_of(amount, rows * top, most, slope, True), portions_of(amount, rows * top, most, slope, False)
    places = jnp.arange(amount)

    def named(sizes, rotation):
        used = int((sizes > 0).sum())
        fixed = max(1, used // 4)
        shifted = fixed + (places - fixed + rotation * (used - fixed)) % max(1, amount - fixed)
        return jnp.zeros((amount,), jnp.int32).at[order[jnp.where(places < fixed, places, shifted)]].set(jnp.asarray(sizes, jnp.int32))

    sizes = jnp.where(number % 4 == 0, named(crowded, number // 4), named(usual, number - number // 4 - 1))
    mixed = jax.random.permutation(jax.random.fold_in(own, 3), amount)
    source_of, receiver = mixed[0:amount // 2 * 2:2], mixed[1:amount // 2 * 2:2]
    room = jnp.minimum(sizes[source_of] - 1, most - sizes[receiver]) // 2
    room = jnp.where((source_of == order[0]) | (receiver == order[0]) | (sizes[receiver] == 0), 0, jnp.maximum(room, 0))
    shifted = jax.random.randint(jax.random.fold_in(own, 4), (amount // 2,), 0, 1 << 20) % (room + 1)
    sizes = sizes.at[source_of].add(-shifted).at[receiver].add(shifted)
    labels = jnp.searchsorted(jnp.cumsum(sizes), jnp.arange(rows * top), side="right").astype(jnp.int32)
    grid = labels.reshape(top, rows).T
    grid = grid[jax.random.permutation(jax.random.fold_in(own, 1), rows)]
    rotation = jax.random.randint(jax.random.fold_in(own, 2), (rows, 1), 0, top)
    return jnp.take_along_axis(grid, (jnp.arange(top)[None, :] + rotation) % top, axis=1)


def portions_of(amount, total, reach, lean, full):
    weights = [(1 << 20) // math.isqrt(rank ** lean) + 1 for rank in range(1, amount + 1)]
    largest = reach if full else min(reach, max(-(-total // amount), total * weights[0] // sum(weights)))
    least = 1 if total - largest >= amount - 1 else 0
    holding, rest = [largest] + [least] * (amount - 1), total - largest - least * (amount - 1)
    while rest > 0:
        movable = [i for i in range(1, amount) if holding[i] < largest] or [i for i in range(1, amount) if holding[i] < reach]
        mass, remaining = sum([weights[i] for i in movable]), rest
        for i in movable:
            more = min(reach - holding[i], max(1, remaining * weights[i] // mass), rest)
            holding[i] = holding[i] + more
            rest = rest - more
    return np.array(holding)


def bell_draw(key, dims, scale, bound, split=(), kind=jnp.bfloat16):
    factor_of = block_scale(key, dims, split, -0.22, 0.18) if split else 1.0
    result = jax.random.normal(key, dims, jnp.float32) * scale * factor_of
    return jnp.minimum(jnp.maximum(result, -bound), bound).astype(kind)


def gaussian_with(key, shape, deviation, most, cuts, heavy, kind=jnp.bfloat16):
    entries = deviation * jax.random.normal(key, shape, jnp.float32)
    if cuts:
        entries = entries * block_scale(key, shape, cuts, -0.22, 0.18)
    return jnp.clip(strengthened(entries, jax.random.fold_in(key, 3), *heavy), -most, most).astype(kind)


def setup_inputs(seed: int = 0) -> dict:
    seeds = jax.random.split(jax.random.key(seed), 8)
    tokens = bell_draw(seeds[0], (TOKENS, D), 1.0, 6.0, ((0, 8), (1, 16)))
    grad_out = bell_draw(seeds[1], (TOKENS, D), 0.1, 0.59765625, ((0, 8), (1, 16)))
    gates = draw_gates(jax.random.fold_in(seeds[7], 71), 0)
    routes_keys = jax.random.split(jax.random.fold_in(seeds[3], 1), TOKENS // TOK_NODE)
    routes_turns = jax.random.permutation(jax.random.fold_in(seeds[3], 3), TOKENS // TOK_NODE)
    routes = jax.vmap(lambda own, number: deal_out(jax.random.fold_in(seeds[3], 2), own, number, TOK_NODE, EXPERTS, TOP, CAP, 2))(routes_keys, routes_turns).reshape((TOKENS, TOP))
    w_gate = gaussian_with(seeds[4], (EXPERTS, D, H), D ** -0.5, 0.09375, ((0, 8), (1, 16)), (1, 2, 16, 2.0))
    w_up = gaussian_with(seeds[5], (EXPERTS, D, H), D ** -0.5, 0.09375, ((0, 8), (1, 16)), (1, 2, 16, 2.0))
    w_down = gaussian_with(seeds[6], (EXPERTS, H, D), H ** -0.5, 0.25, ((0, 8), (2, 16)), (2, 1, 16, 2.0))
    return {"tokens": tokens, "grad_out": grad_out, "gates": gates, "routes": routes, "w_gate": w_gate, "w_up": w_up, "w_down": w_down}


def activation_grads(gate_pre, up_pre, back_hidden, gate_col):
    logistic = jax.nn.sigmoid(gate_pre)
    swished = gate_pre * logistic
    hidden = swished * up_pre
    products = jnp.sum(hidden * back_hidden, axis=-1)
    weight_col = gate_col.astype(jnp.float32)
    scaled = weight_col * back_hidden
    grad_up = (scaled * swished).astype(jnp.bfloat16)
    grad_gate = (scaled * up_pre * logistic * (1.0 + gate_pre * (1.0 - logistic))).astype(jnp.bfloat16)
    weighted = (weight_col * hidden).astype(jnp.bfloat16)
    return weighted, grad_gate, grad_up, products


def slot_tables(flat_routes, expert_count, capacity):
    experts_row = jnp.arange(expert_count, dtype=jnp.int32)
    onehot = (flat_routes[..., None] == experts_row).astype(jnp.int32)
    before = jnp.cumsum(onehot, axis=-2) - onehot
    slot_index = jnp.sum(before * onehot, axis=-1)
    target = flat_routes * capacity + slot_index
    return target


def weight_loads(flat_routes, flat_gates, expert_count):
    experts_row = jnp.arange(expert_count, dtype=jnp.int32)
    onehot = (flat_routes[:, None] == experts_row).astype(jnp.float32)
    return jnp.sum(onehot * flat_gates.astype(jnp.float32)[:, None], axis=0)


def group_sum(partials):
    rounded = lax.optimization_barrier(partials.astype(jnp.bfloat16))
    return jnp.sum(rounded.astype(jnp.float32), axis=0)


def reference(tokens, grad_out, gates, routes, w_gate, w_up, w_down):
    blocks = routes.reshape(N_NODE, TOK_NODE * TOP)
    target = slot_tables(blocks, EXPERTS, CAP)
    weight_sum = weight_loads(routes.reshape(-1), gates.reshape(-1), EXPERTS)
    block_ids = jnp.arange(N_NODE, dtype=jnp.int32)[:, None]
    owners = jnp.broadcast_to(jnp.arange(TOK_NODE * TOP, dtype=jnp.int32)[None, :] // TOP, target.shape)
    token_of = jnp.full((N_NODE, EXPERTS * CAP), TOK_NODE, jnp.int32).at[block_ids, target].set(owners)
    gate_of = jnp.zeros((N_NODE, EXPERTS * CAP), jnp.bfloat16).at[block_ids, target].set(gates.reshape(N_NODE, TOK_NODE * TOP))
    zero_rows = jnp.zeros((N_NODE, 1, D), jnp.bfloat16)
    padded_tokens = jnp.concatenate([tokens.reshape(N_NODE, TOK_NODE, D), zero_rows], axis=1)
    padded_grads = jnp.concatenate([grad_out.reshape(N_NODE, TOK_NODE, D), zero_rows], axis=1)
    group_width = D // N_LOCAL
    slot_rows = N_NODE * CAP

    def one_expert(expert):
        start = (expert * CAP).astype(jnp.int32)
        row_ids = lax.dynamic_slice_in_dim(token_of, start, CAP, 1)
        gate_col = lax.dynamic_slice_in_dim(gate_of, start, CAP, 1).reshape(slot_rows, 1)
        token_rows = padded_tokens[block_ids, row_ids].reshape(slot_rows, D)
        grad_rows = padded_grads[block_ids, row_ids].reshape(slot_rows, D)
        gate_matrix = w_gate[expert]
        up_matrix = w_up[expert]
        down_matrix = w_down[expert]
        token_groups = token_rows.reshape(slot_rows, N_LOCAL, group_width).astype(jnp.float32)
        grad_groups = grad_rows.reshape(slot_rows, N_LOCAL, group_width).astype(jnp.float32)
        gate_groups = gate_matrix.reshape(N_LOCAL, group_width, H).astype(jnp.float32)
        up_groups = up_matrix.reshape(N_LOCAL, group_width, H).astype(jnp.float32)
        down_groups = down_matrix.reshape(H, N_LOCAL, group_width).astype(jnp.float32)
        gate_pre = group_sum(jnp.einsum("rld,ldh->lrh", token_groups, gate_groups, precision=lax.Precision.HIGHEST))
        up_pre = group_sum(jnp.einsum("rld,ldh->lrh", token_groups, up_groups, precision=lax.Precision.HIGHEST))
        back_hidden = group_sum(jnp.einsum("rld,hld->lrh", grad_groups, down_groups, precision=lax.Precision.HIGHEST))
        weighted, grad_gate, grad_up, products = activation_grads(gate_pre, up_pre, back_hidden, gate_col)
        input_rows = (jnp.dot(grad_gate, gate_matrix.T, preferred_element_type=jnp.float32)
                      + jnp.dot(grad_up, up_matrix.T, preferred_element_type=jnp.float32)).astype(jnp.bfloat16)
        grad_wg = jnp.dot(token_rows.T, grad_gate, preferred_element_type=jnp.float32).astype(jnp.bfloat16)
        grad_wu = jnp.dot(token_rows.T, grad_up, preferred_element_type=jnp.float32).astype(jnp.bfloat16)
        grad_wd = jnp.dot(weighted.T, grad_rows, preferred_element_type=jnp.float32).astype(jnp.bfloat16)
        return (input_rows.reshape(N_NODE, CAP, D), products.astype(jnp.bfloat16).reshape(N_NODE, CAP),
                grad_wg, grad_wu, grad_wd)

    input_rows, products, grad_wg, grad_wu, grad_wd = lax.map(one_expert, jnp.arange(EXPERTS, dtype=jnp.int32))
    returned_rows = jnp.transpose(input_rows, (1, 0, 2, 3)).reshape(N_NODE, EXPERTS * CAP, D)
    returned_products = jnp.transpose(products, (1, 0, 2)).reshape(N_NODE, EXPERTS * CAP)
    picked = returned_rows[block_ids, target].reshape(N_NODE, TOK_NODE, TOP, D)
    grad_tokens = jnp.sum(picked.astype(jnp.float32), axis=2).astype(jnp.bfloat16).reshape(N_NODE * TOK_NODE, D)
    grad_gates = returned_products[block_ids, target].reshape(N_NODE * TOK_NODE, TOP)
    loads = weight_sum * (EXPERTS / (TOK_NODE * TOP))
    return grad_tokens, grad_gates, grad_wg, grad_wu, grad_wd, loads
```

```python
import jax
import jax.numpy as jnp
from jax import lax
from jax.sharding import PartitionSpec as P

BF16 = jnp.bfloat16
F32 = jnp.float32


def activation_grads(gate_pre, up_pre, back_hidden, gate_col):
    logistic = jax.nn.sigmoid(gate_pre)
    swished = gate_pre * logistic
    hidden = swished * up_pre
    products = jnp.sum(hidden * back_hidden, axis=-1)
    scaled = gate_col * back_hidden
    grad_up = (scaled * swished).astype(BF16)
    grad_gate = (scaled * up_pre * logistic * (1.0 + gate_pre * (1.0 - logistic))).astype(BF16)
    weighted = (gate_col * hidden).astype(BF16)
    return weighted, grad_gate, grad_up, products


def slot_picks(named, capacity):
    count = named.shape[-1]
    earlier = jnp.arange(count)[:, None] < jnp.arange(count)[None, :]
    slot = jnp.einsum(
        "...s,st->...t", named.astype(BF16), earlier.astype(BF16), preferred_element_type=F32
    )
    slot = jnp.where(named, slot.astype(jnp.int32), -1)
    return (slot[..., None, :] == jnp.arange(capacity, dtype=jnp.int32)[:, None]).astype(BF16)


def on_device(tokens, grad_out, gates, routes, w_gate, w_up, w_down):
    nodes = lax.axis_size("node")
    me = lax.axis_index("node")
    tok_node, width = tokens.shape
    top_k = routes.shape[1]
    own = w_gate.shape[0]
    experts = own * nodes
    capacity = 5 * tok_node * top_k // (4 * experts)
    lanes = -(-(width + experts) // 128) * 128
    spare = lanes - width - experts

    expert_ids = jnp.arange(experts, dtype=jnp.int32)
    choice = routes.T[:, None, :] == expert_ids[None, :, None]
    gate_of = jnp.sum(jnp.where(choice, gates.T[:, None, :].astype(F32), 0.0), axis=0).astype(BF16)
    packed = jnp.concatenate([tokens.T, gate_of, jnp.zeros((spare, tok_node), BF16)], axis=0)
    all_tokens = lax.all_gather(packed, "node", axis=0, tiled=False)
    all_grads = lax.all_gather(grad_out.T, "node", axis=0, tiled=False)

    home_picks = slot_picks(jnp.any(choice, axis=0), capacity)

    all_gates = all_tokens[:, width : width + experts, :]
    loads = jnp.sum(all_gates.astype(F32), axis=(0, 2)) * (experts / (tok_node * top_k * 1.0))
    my_gates = lax.dynamic_slice_in_dim(all_gates, me * own, own, axis=1)
    picks = slot_picks(my_gates > 0, capacity)
    gate_col = jnp.sum(picks.astype(F32) * my_gates[:, :, None, :].astype(F32), axis=-1)
    gate_col = jnp.swapaxes(gate_col, 0, 1).reshape(own, nodes * capacity, 1)

    def rows_of(source):
        rows = jnp.einsum("bjct,bdt->jbcd", picks, source, preferred_element_type=F32)
        return rows.astype(BF16).reshape(own, nodes * capacity, width)

    token_rows = rows_of(all_tokens[:, :width, :])
    grad_rows = rows_of(all_grads)

    gate_pre = jnp.einsum("jrd,jdh->jrh", token_rows, w_gate, preferred_element_type=F32)
    up_pre = jnp.einsum("jrd,jdh->jrh", token_rows, w_up, preferred_element_type=F32)
    back = jnp.einsum("jrd,jhd->jrh", grad_rows, w_down, preferred_element_type=F32)
    gate_full, up_full, back_full = lax.psum(
        (gate_pre.astype(BF16), up_pre.astype(BF16), back.astype(BF16)), "local"
    )
    weighted, grad_gate, grad_up, products = activation_grads(
        gate_full.astype(F32), up_full.astype(F32), back_full.astype(F32), gate_col
    )
    input_rows = (
        jnp.einsum("jrh,jdh->jrd", grad_gate, w_gate, preferred_element_type=F32)
        + jnp.einsum("jrh,jdh->jrd", grad_up, w_up, preferred_element_type=F32)
    ).astype(BF16)
    expert_of = me * own + jnp.arange(own, dtype=jnp.int32)
    marks = expert_of[:, None, None] == expert_ids[None, None, :]
    product_cols = jnp.where(marks, products.astype(BF16)[..., None], jnp.zeros((), BF16))
    back_rows = jnp.concatenate(
        [input_rows, product_cols, jnp.zeros((own, nodes * capacity, spare), BF16)], axis=-1
    )
    back_rows = jnp.swapaxes(back_rows.reshape(own, nodes, capacity, lanes), 0, 1)
    returned = lax.all_to_all(back_rows, "node", split_axis=0, concat_axis=0, tiled=True)

    grad_wg = jnp.einsum(
        "jrd,jrh->jdh", token_rows, grad_gate, preferred_element_type=F32
    ).astype(BF16)
    grad_wu = jnp.einsum(
        "jrd,jrh->jdh", token_rows, grad_up, preferred_element_type=F32
    ).astype(BF16)
    grad_wd = jnp.einsum(
        "jrh,jrd->jhd", weighted, grad_rows, preferred_element_type=F32
    ).astype(BF16)

    home = jnp.einsum(
        "st,sd->dt",
        home_picks.reshape(experts * capacity, tok_node),
        returned.reshape(experts * capacity, lanes),
        preferred_element_type=F32,
    )
    grad_tokens = home[:width].astype(BF16).T
    products_home = home[width : width + experts]
    grad_gates = jnp.sum(jnp.where(choice, products_home[None], 0.0), axis=1).astype(BF16).T
    return (grad_tokens, grad_gates, grad_wg, grad_wu, grad_wd, loads)


def solution(mesh):
    in_specs = (
        P("node", "local"),
        P("node", "local"),
        P("node", None),
        P("node", None),
        P("node", "local", None),
        P("node", "local", None),
        P("node", None, "local"),
    )
    out_specs = (
        P("node", "local"),
        P("node", None),
        P("node", "local", None),
        P("node", "local", None),
        P("node", None, "local"),
        P(),
    )
    return jax.shard_map(
        on_device, mesh=mesh, in_specs=in_specs, out_specs=out_specs, check_vma=False
    )
```

```python
import jax
import jax.numpy as jnp
from jax import lax
from jax.experimental import pallas as pl
from jax.experimental.pallas import tpu as pltpu
from jax.sharding import PartitionSpec as P

BF16 = jnp.bfloat16
F32 = jnp.float32


def activation_grads(gate_pre, up_pre, back_hidden, gate_col):
    logistic = jax.nn.sigmoid(gate_pre)
    swished = gate_pre * logistic
    hidden = swished * up_pre
    products = jnp.sum(hidden * back_hidden, axis=-1)
    scaled = gate_col * back_hidden
    grad_up = (scaled * swished).astype(BF16)
    grad_gate = (scaled * up_pre * logistic * (1.0 + gate_pre * (1.0 - logistic))).astype(BF16)
    weighted = (gate_col * hidden).astype(BF16)
    return weighted, grad_gate, grad_up, products


def slot_picks(named, capacity):
    count = named.shape[-1]
    earlier = jnp.arange(count)[:, None] < jnp.arange(count)[None, :]
    slot = jnp.einsum(
        "...s,st->...t", named.astype(BF16), earlier.astype(BF16), preferred_element_type=F32
    )
    slot = jnp.where(named, slot.astype(jnp.int32), -1)
    return (slot[..., None, :] == jnp.arange(capacity, dtype=jnp.int32)[:, None]).astype(BF16)


def forward_body(tokens_ref, grads_ref, gate_ref, up_ref, down_ref, out_ref):
    quarters, _, rows, lanes = out_ref.shape
    for kind, (left, right) in enumerate(
        ((tokens_ref, gate_ref), (tokens_ref, up_ref), (grads_ref, down_ref))
    ):
        part = jnp.dot(left[0], right[0], preferred_element_type=F32).astype(BF16)
        out_ref[:, kind] = part.reshape(quarters, rows, lanes)


def forward(token_rows, grad_rows, w_gate, w_up, w_down_t, quarters):
    own, slots, width = token_rows.shape
    hidden = w_gate.shape[2]
    lanes = hidden // 2
    share = slots // quarters
    rows = pl.BlockSpec((1, slots, width), lambda e, h: (e, 0, 0))
    weight = pl.BlockSpec((1, width, lanes), lambda e, h: (e, 0, h))
    return pl.pallas_call(
        forward_body,
        grid=(own, hidden // lanes),
        in_specs=[rows, rows, weight, weight, weight],
        out_specs=pl.BlockSpec((quarters, 3, share, lanes), lambda e, h: (e, 0, 0, h)),
        out_shape=jax.ShapeDtypeStruct((own * quarters, 3, share, hidden), BF16),
        name="forward",
    )(token_rows, grad_rows, w_gate, w_up, w_down_t)


def rows_body(grad_gate_ref, grad_up_ref, gate_ref, up_ref, cols_ref, out_ref):
    nodes, _, capacity, _ = out_ref.shape
    slots, extra = cols_ref.shape[1:]
    width = gate_ref.shape[1]
    hidden = gate_ref.shape[2]
    total = jnp.zeros((slots, width), F32)
    for left, right in ((grad_gate_ref, gate_ref), (grad_up_ref, up_ref)):
        total += lax.dot_general(
            left[...].reshape(slots, hidden),
            right[0],
            (((1,), (1,)), ((), ())),
            preferred_element_type=F32,
        )
    out_ref[:, 0, :, :width] = total.astype(BF16).reshape(nodes, capacity, width)
    out_ref[:, 0, :, width:] = cols_ref[0].reshape(nodes, capacity, extra)


def back_rows_of(first, w_gate, w_up, cols, nodes, quarters):
    own, width, hidden = w_gate.shape
    slots, extra = cols.shape[1:]
    share, capacity = slots // quarters, slots // nodes
    grads = [
        pl.BlockSpec((quarters, share, hidden), lambda e, kind=kind: (e, kind, 0))
        for kind in range(2)
    ]
    weight = pl.BlockSpec((1, width, hidden), lambda e: (e, 0, 0))
    return pl.pallas_call(
        rows_body,
        grid=(own,),
        in_specs=[*grads, weight, weight, pl.BlockSpec((1, slots, extra), lambda e: (e, 0, 0))],
        out_specs=pl.BlockSpec((nodes, 1, capacity, width + extra), lambda e: (0, e, 0, 0)),
        out_shape=jax.ShapeDtypeStruct((nodes, own, capacity, width + extra), BF16),
        name="back_rows",
    )(first, first, w_gate, w_up, cols)


def weight_body(rows_ref, *refs):
    half = len(refs) // 2
    for grad_ref, out_ref in zip(refs[:half], refs[half:]):
        slots = rows_ref.shape[1]
        out_ref[0] = lax.dot_general(
            rows_ref[0],
            grad_ref[...].reshape(slots, grad_ref.shape[-1]),
            (((0,), (0,)), ((), ())),
            preferred_element_type=F32,
        ).astype(BF16)


def weight_grads(rows, grads, kinds, quarters):
    own, slots, width = rows.shape
    hidden = grads.shape[-1]
    share = slots // quarters
    lanes = hidden // 2
    out = pl.BlockSpec((1, width, lanes), lambda e, h: (e, 0, h))
    return pl.pallas_call(
        weight_body,
        grid=(own, hidden // lanes),
        in_specs=[pl.BlockSpec((1, slots, width), lambda e, h: (e, 0, 0))]
        + [
            pl.BlockSpec((quarters, share, lanes), lambda e, h, kind=kind: (e, kind, h))
            for kind in range(kinds)
        ],
        out_specs=[out] * kinds,
        out_shape=[jax.ShapeDtypeStruct((own, width, hidden), BF16)] * kinds,
        name="weight_grads",
    )(rows, *([grads] * kinds))


def on_device(tokens, grad_out, gates, routes, w_gate, w_up, w_down):
    nodes = lax.axis_size("node")
    me = lax.axis_index("node")
    tok_node, width = tokens.shape
    top_k = routes.shape[1]
    own = w_gate.shape[0]
    hidden = w_gate.shape[2]
    experts = own * nodes
    capacity = 5 * tok_node * top_k // (4 * experts)
    lanes = -(-(width + experts) // 128) * 128
    spare = lanes - width - experts
    slots = nodes * capacity

    expert_ids = jnp.arange(experts, dtype=jnp.int32)
    choice = routes.T[:, None, :] == expert_ids[None, :, None]
    gate_of = jnp.sum(jnp.where(choice, gates.T[:, None, :].astype(F32), 0.0), axis=0).astype(BF16)
    packed = jnp.concatenate([tokens.T, gate_of, jnp.zeros((spare, tok_node), BF16)], axis=0)
    all_tokens = lax.all_gather(packed, "node", axis=0, tiled=False)
    all_grads = lax.all_to_all(
        jnp.broadcast_to(grad_out.T[None], (nodes, width, tok_node)), "node", 0, 0, tiled=True
    )

    home_picks = slot_picks(jnp.any(choice, axis=0), capacity)

    all_gates = all_tokens[:, width : width + experts, :]
    loads = jnp.sum(all_gates.astype(F32), axis=(0, 2)) * (experts / (tok_node * top_k * 1.0))
    my_gates = lax.dynamic_slice_in_dim(all_gates, me * own, own, axis=1)
    picks = slot_picks(my_gates > 0, capacity)
    gate_col = jnp.sum(picks.astype(F32) * my_gates[:, :, None, :].astype(F32), axis=-1)
    gate_col = jnp.swapaxes(gate_col, 0, 1).reshape(own, slots, 1)

    def rows_of(chosen, source):
        rows = jnp.einsum("bjct,bdt->jbcd", chosen, source, preferred_element_type=F32)
        return rows.astype(BF16).reshape(chosen.shape[1], slots, width)

    devices = lax.axis_size("local")
    place = lax.axis_index("local")
    quarters = devices // own
    share = slots // quarters
    token_rows = rows_of(picks, all_tokens[:, :width, :])
    grad_rows = rows_of(picks, all_grads)
    parts = forward(token_rows, grad_rows, w_gate, w_up, jnp.swapaxes(w_down, 1, 2), quarters)
    parts = parts.reshape(devices, 3 * share, hidden)
    sums = lax.psum_scatter(parts, "local", scatter_dimension=0, tiled=True)
    sums = sums.reshape(3, share, hidden).astype(F32)
    my_gate = lax.dynamic_slice_in_dim(gate_col.reshape(own * slots, 1), place * share, share)
    weighted, grad_gate, grad_up, products = activation_grads(sums[0], sums[1], sums[2], my_gate)
    products = jnp.pad(products.astype(BF16)[None], ((0, 15), (0, hidden - share)))
    first = jnp.concatenate([grad_gate, grad_up, products], axis=0)
    first = lax.all_gather(first, "local", axis=0, tiled=False)
    last = lax.all_gather(weighted, "local", axis=0, tiled=False)

    products = first[:, 2 * share, :share].reshape(own, slots)
    expert_of = me * own + jnp.arange(own, dtype=jnp.int32)
    marks = expert_of[:, None, None] == jnp.arange(experts + spare, dtype=jnp.int32)
    cols = jnp.where(marks, products[..., None], jnp.zeros((), BF16))
    back_rows = back_rows_of(first, w_gate, w_up, cols, nodes, quarters)
    returned = lax.all_to_all(back_rows, "node", split_axis=0, concat_axis=0, tiled=True)
    grad_wg, grad_wu = weight_grads(token_rows, first, 2, quarters)
    home = jnp.einsum(
        "st,sd->dt",
        home_picks.reshape(experts * capacity, tok_node),
        returned.reshape(experts * capacity, lanes),
        preferred_element_type=F32,
    )
    last, grad_wg, grad_wu, home = lax.optimization_barrier((last, grad_wg, grad_wu, home))
    (grad_wd,) = weight_grads(grad_rows, last, 1, quarters)
    grad_wd = jnp.swapaxes(grad_wd, 1, 2)
    grad_tokens = home[:width].astype(BF16).T
    products_home = home[width : width + experts]
    grad_gates = jnp.sum(jnp.where(choice, products_home[None], 0.0), axis=1).astype(BF16).T
    return (grad_tokens, grad_gates, grad_wg, grad_wu, grad_wd, loads)


def solution(mesh):
    in_specs = (
        P("node", "local"),
        P("node", "local"),
        P("node", None),
        P("node", None),
        P("node", "local", None),
        P("node", "local", None),
        P("node", None, "local"),
    )
    out_specs = (
        P("node", "local"),
        P("node", None),
        P("node", "local", None),
        P("node", "local", None),
        P("node", None, "local"),
        P(),
    )
    return jax.shard_map(
        on_device, mesh=mesh, in_specs=in_specs, out_specs=out_specs, check_vma=False
    )
```

```python
import jax
import jax.numpy as jnp
from jax import lax
from jax.experimental import pallas as pl
from jax.experimental.pallas import tpu as pltpu
from jax.sharding import PartitionSpec as P

BF16 = jnp.bfloat16
F32 = jnp.float32


def copy_for_each(array, axis, groups=None):
    devices = len(groups[0]) if groups else lax.axis_size(axis)
    copies = jnp.broadcast_to(array[None], (devices, *array.shape))
    return lax.all_to_all(copies, axis, 0, 0, tiled=True, axis_index_groups=groups)


def activation_grads(gate_pre, up_pre, back_hidden, gate_col):
    logistic = jax.nn.sigmoid(gate_pre)
    swished = gate_pre * logistic
    hidden = swished * up_pre
    products = jnp.sum(hidden * back_hidden, axis=-1)
    scaled = gate_col * back_hidden
    grad_up = (scaled * swished).astype(BF16)
    grad_gate = (scaled * up_pre * logistic * (1.0 + gate_pre * (1.0 - logistic))).astype(BF16)
    weighted = (gate_col * hidden).astype(BF16)
    return weighted, grad_gate, grad_up, products


def slot_picks(named, capacity):
    count = named.shape[-1]
    earlier = jnp.arange(count)[:, None] < jnp.arange(count)[None, :]
    slot = jnp.einsum(
        "...s,st->...t", named.astype(BF16), earlier.astype(BF16), preferred_element_type=F32
    )
    slot = jnp.where(named, slot.astype(jnp.int32), -1)
    return (slot[..., None, :] == jnp.arange(capacity, dtype=jnp.int32)[:, None]).astype(BF16)


def forward_body(tokens_ref, grads_ref, gate_ref, up_ref, down_ref, out_ref):
    quarters, _, rows, lanes = out_ref.shape
    for kind, (left, right) in enumerate(
        ((tokens_ref, gate_ref), (tokens_ref, up_ref), (grads_ref, down_ref))
    ):
        slots = left[...].reshape(quarters * rows, left.shape[-1])
        part = jnp.dot(slots, right[0], preferred_element_type=F32).astype(BF16)
        out_ref[:, kind] = part.reshape(quarters, rows, lanes)


def forward(token_rows, grad_rows, w_gate, w_up, w_down_t, quarters):
    nodes, own, capacity, width = token_rows.shape
    hidden = w_gate.shape[2]
    share = nodes * capacity // quarters
    rows = pl.BlockSpec((nodes, 1, capacity, width), lambda e: (0, e, 0, 0))
    weight = pl.BlockSpec((1, width, hidden), lambda e: (e, 0, 0))
    return pl.pallas_call(
        forward_body,
        grid=(own,),
        in_specs=[rows, rows, weight, weight, weight],
        out_specs=pl.BlockSpec((quarters, 3, share, hidden), lambda e: (e, 0, 0, 0)),
        out_shape=jax.ShapeDtypeStruct((own * quarters, 3, share, hidden), BF16),
        name="forward",
    )(token_rows, grad_rows, w_gate, w_up, w_down_t)


def rows_body(grad_gate_ref, grad_up_ref, gate_ref, up_ref, cols_ref, out_ref):
    nodes, _, capacity, _ = out_ref.shape
    slots, extra = cols_ref.shape[1:]
    width = gate_ref.shape[1]
    hidden = gate_ref.shape[2]
    total = jnp.zeros((slots, width), F32)
    for left, right in ((grad_gate_ref, gate_ref), (grad_up_ref, up_ref)):
        total += lax.dot_general(
            left[...].reshape(slots, hidden),
            right[0],
            (((1,), (1,)), ((), ())),
            preferred_element_type=F32,
        )
    out_ref[:, 0, :, :width] = total.astype(BF16).reshape(nodes, capacity, width)
    out_ref[:, 0, :, width:] = cols_ref[0].reshape(nodes, capacity, extra)


def back_rows_of(first, w_gate, w_up, cols, nodes, quarters):
    own, width, hidden = w_gate.shape
    slots, extra = cols.shape[1:]
    share, capacity = slots // quarters, slots // nodes
    grads = [
        pl.BlockSpec((quarters, share, hidden), lambda e, kind=kind: (e, kind, 0))
        for kind in range(2)
    ]
    weight = pl.BlockSpec((1, width, hidden), lambda e: (e, 0, 0))
    return pl.pallas_call(
        rows_body,
        grid=(own,),
        in_specs=[*grads, weight, weight, pl.BlockSpec((1, slots, extra), lambda e: (e, 0, 0))],
        out_specs=pl.BlockSpec((nodes, 1, capacity, width + extra), lambda e: (0, e, 0, 0)),
        out_shape=jax.ShapeDtypeStruct((nodes, own, capacity, width + extra), BF16),
        name="back_rows",
    )(first, first, w_gate, w_up, cols)


def weight_body(rows_ref, *refs):
    half = len(refs) // 2
    for grad_ref, out_ref in zip(refs[:half], refs[half:]):
        slots = rows_ref.shape[2]
        out_ref[0] = jnp.dot(
            rows_ref[0], grad_ref[...].reshape(slots, grad_ref.shape[-1]), preferred_element_type=F32
        ).astype(BF16)


def weight_grads(rows, grads, kinds, quarters):
    own, width, slots = rows.shape
    hidden = grads.shape[-1]
    share = slots // quarters
    out = pl.BlockSpec((1, width, hidden), lambda e: (e, 0, 0))
    return pl.pallas_call(
        weight_body,
        grid=(own,),
        in_specs=[pl.BlockSpec((1, width, slots), lambda e: (e, 0, 0))]
        + [
            pl.BlockSpec((quarters, share, hidden), lambda e, kind=kind: (e, kind, 0))
            for kind in range(kinds)
        ],
        out_specs=[out] * kinds,
        out_shape=[jax.ShapeDtypeStruct((own, width, hidden), BF16)] * kinds,
        name="weight_grads",
    )(rows, *([grads] * kinds))


def on_device(tokens, grad_out, gates, routes, w_gate, w_up, w_down):
    nodes = lax.axis_size("node")
    me = lax.axis_index("node")
    tok_node, width = tokens.shape
    top_k = routes.shape[1]
    own = w_gate.shape[0]
    hidden = w_gate.shape[2]
    experts = own * nodes
    capacity = 5 * tok_node * top_k // (4 * experts)
    lanes = -(-(width + experts) // 128) * 128
    spare = lanes - width - experts
    slots = nodes * capacity

    expert_ids = jnp.arange(experts, dtype=jnp.int32)
    choice = routes.T[:, None, :] == expert_ids[None, :, None]
    gate_of = jnp.sum(jnp.where(choice, gates.T[:, None, :].astype(F32), 0.0), axis=0).astype(BF16)
    packed = jnp.concatenate([tokens.T, gate_of, jnp.zeros((spare, tok_node), BF16)], axis=0)
    all_tokens = lax.all_gather(packed, "node", axis=0, tiled=False)
    chips = [list(range(core, nodes, 2)) for core in range(2)]
    same = copy_for_each(grad_out.T, "node", chips)
    other = lax.ppermute(same, "node", [(n, n ^ 1) for n in range(nodes)])
    all_grads = jnp.where(me % 2 == 0, jnp.stack([same, other], 1), jnp.stack([other, same], 1))
    all_grads = all_grads.reshape(nodes, width, tok_node)

    home_picks = slot_picks(jnp.any(choice, axis=0), capacity)

    all_gates = all_tokens[:, width : width + experts, :]
    loads = jnp.sum(all_gates.astype(F32), axis=(0, 2)) * (experts / (tok_node * top_k * 1.0))
    my_gates = lax.dynamic_slice_in_dim(all_gates, me * own, own, axis=1)
    picks = slot_picks(my_gates > 0, capacity)
    gate_col = jnp.sum(picks.astype(F32) * my_gates[:, :, None, :].astype(F32), axis=-1)
    gate_col = jnp.swapaxes(gate_col, 0, 1).reshape(own, slots, 1)

    def rows_of(chosen, source):
        rows = jnp.einsum("bjct,bdt->bjcd", chosen, source, preferred_element_type=F32)
        return rows.astype(BF16)

    devices = lax.axis_size("local")
    place = lax.axis_index("local")
    quarters = devices // own
    share = slots // quarters
    token_rows = rows_of(picks, all_tokens[:, :width, :])
    grad_rows = rows_of(picks, all_grads)
    parts = forward(token_rows, grad_rows, w_gate, w_up, jnp.swapaxes(w_down, 1, 2), quarters)
    parts = parts.reshape(devices, 3 * share, hidden)
    sums = lax.psum_scatter(parts, "local", scatter_dimension=0, tiled=True)
    sums = sums.reshape(3, share, hidden).astype(F32)
    my_gate = lax.dynamic_slice_in_dim(gate_col.reshape(own * slots, 1), place * share, share)
    weighted, grad_gate, grad_up, products = activation_grads(sums[0], sums[1], sums[2], my_gate)
    first = jnp.concatenate([grad_gate, grad_up], axis=0)
    first = lax.all_gather(first, "local", axis=0, tiled=False)
    last = lax.all_gather(weighted, "local", axis=0, tiled=False)
    products = copy_for_each(products.astype(BF16)[None], "local").reshape(own, slots)
    expert_of = me * own + jnp.arange(own, dtype=jnp.int32)
    marks = expert_of[:, None, None] == jnp.arange(experts + spare, dtype=jnp.int32)
    cols = jnp.where(marks, products[..., None], jnp.zeros((), BF16))
    back_rows = back_rows_of(first, w_gate, w_up, cols, nodes, quarters)
    returned = lax.all_to_all(back_rows, "node", split_axis=0, concat_axis=0, tiled=True)
    def columns_of(rows):
        return jnp.transpose(rows, (1, 3, 0, 2)).reshape(own, width, slots)

    grad_wg, grad_wu = weight_grads(columns_of(token_rows), first, 2, quarters)
    home = jnp.einsum(
        "st,sd->dt",
        home_picks.reshape(experts * capacity, tok_node),
        returned.reshape(experts * capacity, lanes),
        preferred_element_type=F32,
    )
    grad_tokens = home[:width].astype(BF16).T
    products_home = home[width : width + experts]
    grad_gates = jnp.sum(jnp.where(choice, products_home[None], 0.0), axis=1).astype(BF16).T
    last, grad_wg, grad_wu, grad_tokens, grad_gates = lax.optimization_barrier(
        (last, grad_wg, grad_wu, grad_tokens, grad_gates)
    )
    (grad_wd,) = weight_grads(columns_of(grad_rows), last, 1, quarters)
    grad_wd = jnp.swapaxes(grad_wd, 1, 2)
    return (grad_tokens, grad_gates, grad_wg, grad_wu, grad_wd, loads)


def solution(mesh):
    in_specs = (
        P("node", "local"),
        P("node", "local"),
        P("node", None),
        P("node", None),
        P("node", "local", None),
        P("node", "local", None),
        P("node", None, "local"),
    )
    out_specs = (
        P("node", "local"),
        P("node", None),
        P("node", "local", None),
        P("node", "local", None),
        P("node", None, "local"),
        P(),
    )
    return jax.shard_map(
        on_device, mesh=mesh, in_specs=in_specs, out_specs=out_specs, check_vma=False
    )
```

```python
import jax
import jax.numpy as jnp
from jax import lax
from jax.experimental import pallas as pl
from jax.experimental.pallas import tpu as pltpu
from jax.sharding import Mesh, PartitionSpec as P

BF16 = jnp.bfloat16
F32 = jnp.float32
NODE = ("chip", "core")


def copy_for_each(array, axis):
    copies = jnp.broadcast_to(array[None], (lax.axis_size(axis), *array.shape))
    return lax.all_to_all(copies, axis, 0, 0, tiled=True)


def activation_grads(gate_pre, up_pre, back_hidden, gate_col):
    logistic = jax.nn.sigmoid(gate_pre)
    swished = gate_pre * logistic
    hidden = swished * up_pre
    products = jnp.sum(hidden * back_hidden, axis=-1)
    scaled = gate_col * back_hidden
    grad_up = (scaled * swished).astype(BF16)
    grad_gate = (scaled * up_pre * logistic * (1.0 + gate_pre * (1.0 - logistic))).astype(BF16)
    weighted = (gate_col * hidden).astype(BF16)
    return weighted, grad_gate, grad_up, products


def slot_picks(named, capacity):
    count = named.shape[-1]
    earlier = jnp.arange(count)[:, None] < jnp.arange(count)[None, :]
    slot = jnp.einsum(
        "...s,st->...t", named.astype(BF16), earlier.astype(BF16), preferred_element_type=F32
    )
    slot = jnp.where(named, slot.astype(jnp.int32), -1)
    return (slot[..., None, :] == jnp.arange(capacity, dtype=jnp.int32)[:, None]).astype(BF16)


def ring_shift(array, ring, step):
    pairs = []
    for y in range(4):
        for z in range(4):
            target = ((y + step) % 4, z) if ring == "y" else (y, (z + step) % 4)
            pairs.append((4 * y + z, 4 * target[0] + target[1]))
    return lax.ppermute(array, "local", pairs)


def ring_gather(parts, rings):
    half = parts[0].shape[0] // 2
    count = range(len(parts))
    left = [ring_shift(parts[i], rings[i], 1) for i in count]
    right = [ring_shift(parts[i], rings[i], -1) for i in count]
    far_a = [ring_shift(left[i][:half], rings[i], 1) for i in count]
    far_b = [ring_shift(right[i][half:], rings[i], -1) for i in count]
    index = lax.axis_index("local")
    result = []
    for i in count:
        place = index // 4 if rings[i] == "y" else index % 4
        whole = jnp.zeros((4, *parts[i].shape), parts[i].dtype)
        across = jnp.concatenate([far_a[i], far_b[i]], axis=0)
        for value, step in ((parts[i], 0), (left[i], -1), (right[i], 1), (across, 2)):
            whole = lax.dynamic_update_index_in_dim(whole, value, (place + step) % 4, 0)
        result.append(whole)
    return result


def ring_scatter(parts, rings):
    half = parts[0].shape[1] // 2
    count = range(len(parts))
    index = lax.axis_index("local")
    place = [index // 4 if ring == "y" else index % 4 for ring in rings]

    def quarter(i, step):
        return lax.dynamic_index_in_dim(parts[i], (place[i] + step) % 4, 0, keepdims=False)

    across = [quarter(i, 2) for i in count]
    left = [ring_shift(across[i][:half], rings[i], 1) for i in count]
    right = [ring_shift(across[i][half:], rings[i], -1) for i in count]
    up = [quarter(i, 1) for i in count]
    up = [jnp.concatenate([up[i][:half] + left[i], up[i][half:]], axis=0) for i in count]
    down = [quarter(i, -1) for i in count]
    down = [jnp.concatenate([down[i][:half], down[i][half:] + right[i]], axis=0) for i in count]
    up = [ring_shift(up[i], rings[i], 1) for i in count]
    down = [ring_shift(down[i], rings[i], -1) for i in count]
    return [
        (quarter(i, 0).astype(F32) + up[i].astype(F32) + down[i].astype(F32)).astype(BF16)
        for i in count
    ]


def plane_scatter(low, high):
    kinds, rows, lanes = low.shape[2:]
    sums = [part.reshape(4, 4 * kinds, rows, lanes) for part in (low, high)]
    sums = ring_scatter(sums, ("y", "z"))
    sums = [part.reshape(4, 2 * kinds, rows // 2, lanes) for part in sums]
    sums = ring_scatter(sums, ("z", "y"))
    return [part.reshape(kinds, rows, lanes) for part in sums]


def plane_gather(part):
    rows, lanes = part.shape
    halves = [part[:, : lanes // 2], part[:, lanes // 2 :]]
    halves = [half.reshape(2, rows // 2, lanes // 2) for half in halves]
    halves = ring_gather(halves, ("z", "y"))
    halves = [half.reshape(4, rows, lanes // 2) for half in halves]
    return ring_gather(halves, ("y", "z"))


def forward_body(tokens_ref, grads_ref, gate_ref, up_ref, down_ref, out_ref, low_ref, high_ref):
    quarters, _, rows, lanes = out_ref.shape
    part_lanes = low_ref.shape[-1]
    for kind, (left, right) in enumerate(
        ((tokens_ref, gate_ref), (tokens_ref, up_ref), (grads_ref, down_ref))
    ):
        slots = left[...].reshape(quarters * rows, left.shape[-1])
        part = jnp.dot(slots, right[0], preferred_element_type=F32).astype(BF16)
        part = part.reshape(quarters, rows, part.shape[-1])
        out_ref[:, kind] = part[..., :lanes]
        low_ref[0, :, kind] = part[..., lanes : lanes + part_lanes]
        high_ref[:, 0, kind] = part[..., lanes + part_lanes :]


def forward(token_rows, grad_rows, w_gate, w_up, w_down_t, quarters):
    nodes, own, capacity, width = token_rows.shape
    hidden = w_gate.shape[2]
    lanes = hidden // 4
    share = nodes * capacity // quarters
    rows = pl.BlockSpec((nodes, 1, capacity, width), lambda e: (0, e, 0, 0))
    weight = pl.BlockSpec((1, width, hidden), lambda e: (e, 0, 0))
    first = hidden - 2 * lanes
    return pl.pallas_call(
        forward_body,
        grid=(own,),
        in_specs=[rows, rows, weight, weight, weight],
        out_specs=[
            pl.BlockSpec((quarters, 3, share, first), lambda e: (e, 0, 0, 0)),
            pl.BlockSpec((1, quarters, 3, share, lanes), lambda e: (e, 0, 0, 0, 0)),
            pl.BlockSpec((quarters, 1, 3, share, lanes), lambda e: (0, e, 0, 0, 0)),
        ],
        out_shape=[
            jax.ShapeDtypeStruct((own * quarters, 3, share, first), BF16),
            jax.ShapeDtypeStruct((own, quarters, 3, share, lanes), BF16),
            jax.ShapeDtypeStruct((quarters, own, 3, share, lanes), BF16),
        ],
        name="forward",
    )(token_rows, grad_rows, w_gate, w_up, w_down_t)


def rows_body(grad_gate_ref, grad_up_ref, gate_ref, up_ref, cols_ref, out_ref):
    nodes, _, capacity, _ = out_ref.shape
    slots, extra = cols_ref.shape[1:]
    width = gate_ref.shape[1]
    hidden = gate_ref.shape[2]
    total = jnp.zeros((slots, width), F32)
    for left, right in ((grad_gate_ref, gate_ref), (grad_up_ref, up_ref)):
        total += lax.dot_general(
            left[...].reshape(slots, hidden),
            right[0],
            (((1,), (1,)), ((), ())),
            preferred_element_type=F32,
        )
    out_ref[:, 0, :, :width] = total.astype(BF16).reshape(nodes, capacity, width)
    out_ref[:, 0, :, width:] = cols_ref[0].reshape(nodes, capacity, extra)


def back_rows_of(first, w_gate, w_up, cols, nodes, quarters):
    own, width, hidden = w_gate.shape
    slots, extra = cols.shape[1:]
    share, capacity = slots // quarters, slots // nodes
    grads = [
        pl.BlockSpec((quarters, share, hidden), lambda e, kind=kind: (e, kind, 0))
        for kind in range(2)
    ]
    weight = pl.BlockSpec((1, width, hidden), lambda e: (e, 0, 0))
    return pl.pallas_call(
        rows_body,
        grid=(own,),
        in_specs=[*grads, weight, weight, pl.BlockSpec((1, slots, extra), lambda e: (e, 0, 0))],
        out_specs=pl.BlockSpec((nodes, 1, capacity, width + extra), lambda e: (0, e, 0, 0)),
        out_shape=jax.ShapeDtypeStruct((nodes, own, capacity, width + extra), BF16),
        name="back_rows",
    )(first, first, w_gate, w_up, cols)


def weight_body(rows_ref, *refs):
    half = len(refs) // 2
    for grad_ref, out_ref in zip(refs[:half], refs[half:]):
        slots = rows_ref.shape[2]
        out_ref[0] = jnp.dot(
            rows_ref[0], grad_ref[...].reshape(slots, grad_ref.shape[-1]), preferred_element_type=F32
        ).astype(BF16)


def weight_grads(rows, grads, kinds, quarters):
    own, width, slots = rows.shape
    hidden = grads.shape[-1]
    share = slots // quarters
    out = pl.BlockSpec((1, width, hidden), lambda e: (e, 0, 0))
    return pl.pallas_call(
        weight_body,
        grid=(own,),
        in_specs=[pl.BlockSpec((1, width, slots), lambda e: (e, 0, 0))]
        + [
            pl.BlockSpec((quarters, share, hidden), lambda e, kind=kind: (e, kind, 0))
            for kind in range(kinds)
        ],
        out_specs=[out] * kinds,
        out_shape=[jax.ShapeDtypeStruct((own, width, hidden), BF16)] * kinds,
        name="weight_grads",
    )(rows, *([grads] * kinds))


def down_body(rows_ref, low_ref, high_ref, out_ref):
    lanes = low_ref.shape[-1]
    slots = rows_ref.shape[2]
    for half, half_ref in enumerate((low_ref, high_ref)):
        out_ref[0, :, half * lanes : (half + 1) * lanes] = jnp.dot(
            rows_ref[0], half_ref[...].reshape(slots, lanes), preferred_element_type=F32
        ).astype(BF16)


def down_grads(rows, low, high):
    own, width, slots = rows.shape
    share, lanes = low.shape[2:]
    return pl.pallas_call(
        down_body,
        grid=(own,),
        in_specs=[
            pl.BlockSpec((1, width, slots), lambda e: (e, 0, 0)),
            pl.BlockSpec((1, 4, share, lanes), lambda e: (e, 0, 0, 0)),
            pl.BlockSpec((4, 1, share, lanes), lambda e: (0, e, 0, 0)),
        ],
        out_specs=pl.BlockSpec((1, width, 2 * lanes), lambda e: (e, 0, 0)),
        out_shape=jax.ShapeDtypeStruct((own, width, 2 * lanes), BF16),
        name="down_grads",
    )(rows, low, high)


def on_device(tokens, grad_out, gates, routes, w_gate, w_up, w_down):
    nodes = lax.axis_size(NODE)
    me = lax.axis_index(NODE)
    tok_node, width = tokens.shape
    top_k = routes.shape[1]
    own = w_gate.shape[0]
    hidden = w_gate.shape[2]
    experts = own * nodes
    capacity = 5 * tok_node * top_k // (4 * experts)
    lanes = -(-(width + experts) // 128) * 128
    spare = lanes - width - experts
    slots = nodes * capacity

    expert_ids = jnp.arange(experts, dtype=jnp.int32)
    choice = routes.T[:, None, :] == expert_ids[None, :, None]
    gate_of = jnp.sum(jnp.where(choice, gates.T[:, None, :].astype(F32), 0.0), axis=0).astype(BF16)
    packed = jnp.concatenate([tokens.T, gate_of, jnp.zeros((spare, tok_node), BF16)], axis=0)
    all_tokens = lax.all_gather(packed, NODE, axis=0, tiled=False)
    first_core = lax.axis_index("core") == 0
    same = copy_for_each(grad_out.T, "chip")
    other = lax.ppermute(same, "core", [(0, 1), (1, 0)])
    all_grads = jnp.where(first_core, jnp.stack([same, other], 1), jnp.stack([other, same], 1))
    all_grads = all_grads.reshape(nodes, width, tok_node)

    all_gates = all_tokens[:, width : width + experts, :]
    loads = jnp.sum(all_gates.astype(F32), axis=(0, 2)) * (experts / (tok_node * top_k * 1.0))
    my_gates = lax.dynamic_slice_in_dim(all_gates, me * own, own, axis=1)
    picks = slot_picks(my_gates > 0, capacity)
    gate_col = jnp.sum(picks.astype(F32) * my_gates[:, :, None, :].astype(F32), axis=-1)
    gate_col = jnp.swapaxes(gate_col, 0, 1).reshape(own, slots, 1)

    def rows_of(chosen, source):
        rows = jnp.einsum("bjct,bdt->bjcd", chosen, source, preferred_element_type=F32)
        return rows.astype(BF16)

    devices = lax.axis_size("local")
    place = lax.axis_index("local")
    quarters = devices // own
    share = slots // quarters
    token_rows = rows_of(picks, all_tokens[:, :width, :])
    grad_rows = rows_of(picks, all_grads)
    parts, low, high = forward(
        token_rows, grad_rows, w_gate, w_up, jnp.swapaxes(w_down, 1, 2), quarters
    )
    parts = parts.reshape(devices, 3 * share, parts.shape[-1])
    def columns_of(rows):
        return jnp.transpose(rows, (1, 3, 0, 2)).reshape(own, width, slots)

    token_columns, grad_columns = columns_of(token_rows), columns_of(grad_rows)
    sums = lax.psum_scatter(parts, "local", scatter_dimension=0, tiled=True)
    sums, token_columns, grad_columns = lax.optimization_barrier(
        (sums, token_columns, grad_columns)
    )
    sums = jnp.concatenate([sums.reshape(3, share, -1), *plane_scatter(low, high)], axis=-1)
    sums = sums.astype(F32)
    my_gate = lax.dynamic_slice_in_dim(gate_col.reshape(own * slots, 1), place * share, share)
    weighted, grad_gate, grad_up, products = activation_grads(sums[0], sums[1], sums[2], my_gate)
    first = jnp.concatenate([grad_gate, grad_up], axis=0)
    first = lax.all_gather(first, "local", axis=0, tiled=False)
    grad_wd = jnp.swapaxes(down_grads(grad_columns, *plane_gather(weighted)), 1, 2)
    products = copy_for_each(products.astype(BF16)[None], "local").reshape(own, slots)
    expert_of = me * own + jnp.arange(own, dtype=jnp.int32)
    marks = expert_of[:, None, None] == jnp.arange(experts + spare, dtype=jnp.int32)
    cols = jnp.where(marks, products[..., None], jnp.zeros((), BF16))
    first, grad_wd = lax.optimization_barrier((first, grad_wd))
    back_rows = back_rows_of(first, w_gate, w_up, cols, nodes, quarters)
    token_sums = jnp.einsum("bjct,bjcd->bdt", picks, back_rows, preferred_element_type=F32)
    token_sums = token_sums.astype(BF16).reshape(nodes // 2, 2, lanes, tok_node)
    kept = jnp.where(first_core, token_sums[:, 0], token_sums[:, 1])
    given = jnp.where(first_core, token_sums[:, 1], token_sums[:, 0])
    taken = lax.ppermute(given, "core", [(0, 1), (1, 0)])
    token_sums = (kept.astype(F32) + taken.astype(F32)).astype(BF16)
    token_sums = lax.all_to_all(token_sums, "chip", 0, 0, tiled=True)
    home = jnp.sum(token_sums.astype(F32), axis=0)

    grad_wg, grad_wu = weight_grads(token_columns, first, 2, quarters)
    grad_tokens = home[:width].astype(BF16).T
    products_home = home[width : width + experts]
    grad_gates = jnp.sum(jnp.where(choice, products_home[None], 0.0), axis=1).astype(BF16).T
    return (grad_tokens, grad_gates, grad_wg, grad_wu, grad_wd, loads)


def solution(mesh):
    nodes, devices = mesh.shape["node"], mesh.shape["local"]
    fine = Mesh(mesh.devices.reshape(nodes // 2, 2, devices), ("chip", "core", "local"))
    in_specs = (
        P(NODE, "local"),
        P(NODE, "local"),
        P(NODE, None),
        P(NODE, None),
        P(NODE, "local", None),
        P(NODE, "local", None),
        P(NODE, None, "local"),
    )
    out_specs = (
        P(NODE, "local"),
        P(NODE, None),
        P(NODE, "local", None),
        P(NODE, "local", None),
        P(NODE, None, "local"),
        P(),
    )
    return jax.shard_map(
        on_device, mesh=fine, in_specs=in_specs, out_specs=out_specs, check_vma=False
    )
```

```python
import jax
import jax.numpy as jnp
from jax import lax
from jax.experimental import pallas as pl
from jax.experimental.pallas import tpu as pltpu
from jax.sharding import Mesh, PartitionSpec as P

BF16 = jnp.bfloat16
F32 = jnp.float32
NODE = ("chip", "core")


def copy_for_each(array, axis):
    copies = jnp.broadcast_to(array[None], (lax.axis_size(axis), *array.shape))
    return lax.all_to_all(copies, axis, 0, 0, tiled=True)


def activation_grads(gate_pre, up_pre, back_hidden, gate_col):
    logistic = jax.nn.sigmoid(gate_pre)
    swished = gate_pre * logistic
    hidden = swished * up_pre
    products = jnp.sum(hidden * back_hidden, axis=-1)
    scaled = gate_col * back_hidden
    grad_up = (scaled * swished).astype(BF16)
    grad_gate = (scaled * up_pre * logistic * (1.0 + gate_pre * (1.0 - logistic))).astype(BF16)
    weighted = (gate_col * hidden).astype(BF16)
    return weighted, grad_gate, grad_up, products


def slot_picks(named, capacity):
    count = named.shape[-1]
    earlier = jnp.arange(count)[:, None] < jnp.arange(count)[None, :]
    slot = jnp.einsum(
        "...s,st->...t", named.astype(BF16), earlier.astype(BF16), preferred_element_type=F32
    )
    slot = jnp.where(named, slot.astype(jnp.int32), -1)
    return (slot[..., None, :] == jnp.arange(capacity, dtype=jnp.int32)[:, None]).astype(BF16)


def ring_shift(array, ring, step):
    pairs = []
    for y in range(4):
        for z in range(4):
            target = ((y + step) % 4, z) if ring == "y" else (y, (z + step) % 4)
            pairs.append((4 * y + z, 4 * target[0] + target[1]))
    return lax.ppermute(array, "local", pairs)


def ring_gather(parts, rings):
    half = parts[0].shape[0] // 2
    count = range(len(parts))
    left = [ring_shift(parts[i], rings[i], 1) for i in count]
    right = [ring_shift(parts[i], rings[i], -1) for i in count]
    far_a = [ring_shift(left[i][:half], rings[i], 1) for i in count]
    far_b = [ring_shift(right[i][half:], rings[i], -1) for i in count]
    index = lax.axis_index("local")
    result = []
    for i in count:
        place = index // 4 if rings[i] == "y" else index % 4
        whole = jnp.zeros((4, *parts[i].shape), parts[i].dtype)
        across = jnp.concatenate([far_a[i], far_b[i]], axis=0)
        for value, step in ((parts[i], 0), (left[i], -1), (right[i], 1), (across, 2)):
            whole = lax.dynamic_update_index_in_dim(whole, value, (place + step) % 4, 0)
        result.append(whole)
    return result


def ring_scatter(parts, rings):
    half = parts[0].shape[1] // 2
    count = range(len(parts))
    index = lax.axis_index("local")
    place = [index // 4 if ring == "y" else index % 4 for ring in rings]

    def quarter(i, step):
        return lax.dynamic_index_in_dim(parts[i], (place[i] + step) % 4, 0, keepdims=False)

    across = [quarter(i, 2) for i in count]
    left = [ring_shift(across[i][:half], rings[i], 1) for i in count]
    right = [ring_shift(across[i][half:], rings[i], -1) for i in count]
    up = [quarter(i, 1) for i in count]
    up = [jnp.concatenate([up[i][:half] + left[i], up[i][half:]], axis=0) for i in count]
    down = [quarter(i, -1) for i in count]
    down = [jnp.concatenate([down[i][:half], down[i][half:] + right[i]], axis=0) for i in count]
    up = [ring_shift(up[i], rings[i], 1) for i in count]
    down = [ring_shift(down[i], rings[i], -1) for i in count]
    return [
        (quarter(i, 0).astype(F32) + up[i].astype(F32) + down[i].astype(F32)).astype(BF16)
        for i in count
    ]


def plane_scatter(low, high):
    kinds, rows, lanes = low.shape[2:]
    sums = [part.reshape(4, 4 * kinds, rows, lanes) for part in (low, high)]
    sums = ring_scatter(sums, ("y", "z"))
    sums = [part.reshape(4, 2 * kinds, rows // 2, lanes) for part in sums]
    sums = ring_scatter(sums, ("z", "y"))
    return [part.reshape(kinds, rows, lanes) for part in sums]


def plane_gather(part):
    rows, lanes = part.shape
    halves = [part[:, : lanes // 2], part[:, lanes // 2 :]]
    halves = [half.reshape(2, rows // 2, lanes // 2) for half in halves]
    halves = ring_gather(halves, ("z", "y"))
    halves = [half.reshape(4, rows, lanes // 2) for half in halves]
    return ring_gather(halves, ("y", "z"))


def cost(flops, size):
    return pl.CostEstimate(flops=flops, bytes_accessed=size, transcendentals=0)


def forward_body(tokens_ref, grads_ref, gate_ref, up_ref, down_ref, out_ref, low_ref, high_ref):
    quarters, _, rows, lanes = out_ref.shape
    part_lanes = low_ref.shape[-1]
    for kind, (left, right) in enumerate(
        ((tokens_ref, gate_ref), (tokens_ref, up_ref), (grads_ref, down_ref))
    ):
        slots = left[...].reshape(quarters * rows, left.shape[-1])
        part = jnp.dot(slots, right[0], preferred_element_type=F32).astype(BF16)
        part = part.reshape(quarters, rows, part.shape[-1])
        out_ref[:, kind] = part[..., :lanes]
        low_ref[0, :, kind] = part[..., lanes : lanes + part_lanes]
        high_ref[:, 0, kind] = part[..., lanes + part_lanes :]


def forward(token_rows, grad_rows, w_gate, w_up, w_down_t, quarters):
    nodes, own, capacity, width = token_rows.shape
    hidden = w_gate.shape[2]
    lanes = hidden // 4
    share = nodes * capacity // quarters
    rows = pl.BlockSpec((nodes, 1, capacity, width), lambda e: (0, e, 0, 0))
    weight = pl.BlockSpec((1, width, hidden), lambda e: (e, 0, 0))
    first = hidden - 2 * lanes
    return pl.pallas_call(
        forward_body,
        grid=(own,),
        in_specs=[rows, rows, weight, weight, weight],
        out_specs=[
            pl.BlockSpec((quarters, 3, share, first), lambda e: (e, 0, 0, 0)),
            pl.BlockSpec((1, quarters, 3, share, lanes), lambda e: (e, 0, 0, 0, 0)),
            pl.BlockSpec((quarters, 1, 3, share, lanes), lambda e: (0, e, 0, 0, 0)),
        ],
        out_shape=[
            jax.ShapeDtypeStruct((own * quarters, 3, share, first), BF16),
            jax.ShapeDtypeStruct((own, quarters, 3, share, lanes), BF16),
            jax.ShapeDtypeStruct((quarters, own, 3, share, lanes), BF16),
        ],
        name="forward",
        cost_estimate=cost(6 * own * nodes * capacity * width * hidden, 32 << 20),
    )(token_rows, grad_rows, w_gate, w_up, w_down_t)


def rows_body(grad_gate_ref, grad_up_ref, gate_ref, up_ref, cols_ref, out_ref):
    nodes, _, capacity, _ = out_ref.shape
    slots, extra = cols_ref.shape[1:]
    width = gate_ref.shape[1]
    hidden = gate_ref.shape[2]
    total = jnp.zeros((slots, width), F32)
    for left, right in ((grad_gate_ref, gate_ref), (grad_up_ref, up_ref)):
        total += lax.dot_general(
            left[...].reshape(slots, hidden),
            right[0],
            (((1,), (1,)), ((), ())),
            preferred_element_type=F32,
        )
    out_ref[:, 0, :, :width] = total.astype(BF16).reshape(nodes, capacity, width)
    out_ref[:, 0, :, width:] = cols_ref[0].reshape(nodes, capacity, extra)


def back_rows_of(first, w_gate, w_up, cols, nodes, quarters):
    own, width, hidden = w_gate.shape
    slots, extra = cols.shape[1:]
    share, capacity = slots // quarters, slots // nodes
    grads = [
        pl.BlockSpec((quarters, share, hidden), lambda e, kind=kind: (e, kind, 0))
        for kind in range(2)
    ]
    weight = pl.BlockSpec((1, width, hidden), lambda e: (e, 0, 0))
    return pl.pallas_call(
        rows_body,
        grid=(own,),
        in_specs=[*grads, weight, weight, pl.BlockSpec((1, slots, extra), lambda e: (e, 0, 0))],
        out_specs=pl.BlockSpec((nodes, 1, capacity, width + extra), lambda e: (0, e, 0, 0)),
        out_shape=jax.ShapeDtypeStruct((nodes, own, capacity, width + extra), BF16),
        name="back_rows",
        cost_estimate=cost(4 * own * slots * width * hidden, 20 << 20),
    )(first, first, w_gate, w_up, cols)


def weight_body(rows_ref, *refs):
    half = len(refs) // 2
    for grad_ref, out_ref in zip(refs[:half], refs[half:]):
        slots = rows_ref.shape[2]
        out_ref[0] = jnp.dot(
            rows_ref[0], grad_ref[...].reshape(slots, grad_ref.shape[-1]), preferred_element_type=F32
        ).astype(BF16)


def weight_grads(rows, grads, kinds, quarters):
    own, width, slots = rows.shape
    hidden = grads.shape[-1]
    share = slots // quarters
    out = pl.BlockSpec((1, width, hidden), lambda e: (e, 0, 0))
    return pl.pallas_call(
        weight_body,
        grid=(own,),
        in_specs=[pl.BlockSpec((1, width, slots), lambda e: (e, 0, 0))]
        + [
            pl.BlockSpec((quarters, share, hidden), lambda e, kind=kind: (e, kind, 0))
            for kind in range(kinds)
        ],
        out_specs=[out] * kinds,
        out_shape=[jax.ShapeDtypeStruct((own, width, hidden), BF16)] * kinds,
        name="weight_grads",
        cost_estimate=cost(2 * kinds * own * slots * width * hidden, 20 << 20),
    )(rows, *([grads] * kinds))


def down_body(rows_ref, low_ref, high_ref, out_ref):
    lanes = low_ref.shape[-1]
    slots = rows_ref.shape[2]
    for half, half_ref in enumerate((low_ref, high_ref)):
        out_ref[0, :, half * lanes : (half + 1) * lanes] = jnp.dot(
            rows_ref[0], half_ref[...].reshape(slots, lanes), preferred_element_type=F32
        ).astype(BF16)


def down_grads(rows, low, high):
    own, width, slots = rows.shape
    share, lanes = low.shape[2:]
    return pl.pallas_call(
        down_body,
        grid=(own,),
        in_specs=[
            pl.BlockSpec((1, width, slots), lambda e: (e, 0, 0)),
            pl.BlockSpec((1, 4, share, lanes), lambda e: (e, 0, 0, 0)),
            pl.BlockSpec((4, 1, share, lanes), lambda e: (0, e, 0, 0)),
        ],
        out_specs=pl.BlockSpec((1, width, 2 * lanes), lambda e: (e, 0, 0)),
        out_shape=jax.ShapeDtypeStruct((own, width, 2 * lanes), BF16),
        name="down_grads",
        cost_estimate=cost(4 * own * slots * width * lanes, 11 << 20),
    )(rows, low, high)


def on_device(tokens, grad_out, gates, routes, w_gate, w_up, w_down):
    nodes = lax.axis_size(NODE)
    me = lax.axis_index(NODE)
    tok_node, width = tokens.shape
    top_k = routes.shape[1]
    own = w_gate.shape[0]
    hidden = w_gate.shape[2]
    experts = own * nodes
    capacity = 5 * tok_node * top_k // (4 * experts)
    lanes = width + experts
    slots = nodes * capacity

    expert_ids = jnp.arange(experts, dtype=jnp.int32)
    choice = routes.T[:, None, :] == expert_ids[None, :, None]
    gate_of = jnp.sum(jnp.where(choice, gates.T[:, None, :].astype(F32), 0.0), axis=0).astype(BF16)
    packed = jnp.concatenate([tokens.T, gate_of], axis=0)
    all_tokens = lax.all_gather(packed, NODE, axis=0, tiled=False)
    first_core = lax.axis_index("core") == 0
    same = copy_for_each(grad_out.T, "chip")
    other = lax.ppermute(same, "core", [(0, 1), (1, 0)])
    all_grads = jnp.where(first_core, jnp.stack([same, other], 1), jnp.stack([other, same], 1))
    all_grads = all_grads.reshape(nodes, width, tok_node)

    all_gates = all_tokens[:, width : width + experts, :]
    loads = jnp.sum(all_gates.astype(F32), axis=(0, 2)) * (experts / (tok_node * top_k * 1.0))
    my_gates = lax.dynamic_slice_in_dim(all_tokens, width + me * own, own, axis=1)
    picks = slot_picks(my_gates > 0, capacity)
    gate_col = jnp.sum(picks.astype(F32) * my_gates[:, :, None, :].astype(F32), axis=-1)
    gate_col = jnp.swapaxes(gate_col, 0, 1).reshape(own, slots, 1)

    def rows_of(chosen, source):
        rows = jnp.einsum("bjct,bdt->bjcd", chosen, source, preferred_element_type=F32)
        return rows.astype(BF16)

    devices = lax.axis_size("local")
    place = lax.axis_index("local")
    quarters = devices // own
    share = slots // quarters
    token_rows = rows_of(picks, all_tokens[:, :width, :])
    grad_rows = rows_of(picks, all_grads)
    parts, low, high = forward(
        token_rows, grad_rows, w_gate, w_up, jnp.swapaxes(w_down, 1, 2), quarters
    )
    parts = parts.reshape(devices, 3 * share, parts.shape[-1])
    def columns_of(rows):
        return jnp.transpose(rows, (1, 3, 0, 2)).reshape(own, width, slots)

    token_columns, grad_columns = columns_of(token_rows), columns_of(grad_rows)
    sums = lax.psum_scatter(parts, "local", scatter_dimension=0, tiled=True)
    sums, token_columns, grad_columns = lax.optimization_barrier(
        (sums, token_columns, grad_columns)
    )
    sums = jnp.concatenate([sums.reshape(3, share, -1), *plane_scatter(low, high)], axis=-1)
    sums = sums.astype(F32)
    my_gate = lax.dynamic_slice_in_dim(gate_col.reshape(own * slots, 1), place * share, share)
    weighted, grad_gate, grad_up, products = activation_grads(sums[0], sums[1], sums[2], my_gate)
    first = jnp.concatenate([grad_gate, grad_up], axis=0)
    first = lax.all_gather(first, "local", axis=0, tiled=False)
    grad_wd = jnp.swapaxes(down_grads(grad_columns, *plane_gather(weighted)), 1, 2)
    products = copy_for_each(products.astype(BF16)[None], "local").reshape(own, slots)
    expert_of = me * own + jnp.arange(own, dtype=jnp.int32)
    marks = expert_of[:, None, None] == expert_ids
    cols = jnp.where(marks, products[..., None], jnp.zeros((), BF16))
    first, grad_wd = lax.optimization_barrier((first, grad_wd))
    back_rows = back_rows_of(first, w_gate, w_up, cols, nodes, quarters)
    token_sums = jnp.einsum("bjct,bjcd->bdt", picks, back_rows, preferred_element_type=F32)
    token_sums = token_sums.astype(BF16).reshape(nodes // 2, 2, lanes, tok_node)
    kept = jnp.where(first_core, token_sums[:, 0], token_sums[:, 1])
    given = jnp.where(first_core, token_sums[:, 1], token_sums[:, 0])
    taken = lax.ppermute(given, "core", [(0, 1), (1, 0)])
    token_sums = (kept.astype(F32) + taken.astype(F32)).astype(BF16)
    token_sums = lax.all_to_all(token_sums, "chip", 0, 0, tiled=True)
    home = jnp.sum(token_sums.astype(F32), axis=0)

    grad_wg, grad_wu = weight_grads(token_columns, first, 2, quarters)
    grad_tokens = home[:width].astype(BF16).T
    products_home = home[width : width + experts]
    grad_gates = jnp.sum(jnp.where(choice, products_home[None], 0.0), axis=1).astype(BF16).T
    return (grad_tokens, grad_gates, grad_wg, grad_wu, grad_wd, loads)


def solution(mesh):
    nodes, devices = mesh.shape["node"], mesh.shape["local"]
    fine = Mesh(mesh.devices.reshape(nodes // 2, 2, devices), ("chip", "core", "local"))
    in_specs = (
        P(NODE, "local"),
        P(NODE, "local"),
        P(NODE, None),
        P(NODE, None),
        P(NODE, "local", None),
        P(NODE, "local", None),
        P(NODE, None, "local"),
    )
    out_specs = (
        P(NODE, "local"),
        P(NODE, None),
        P(NODE, "local", None),
        P(NODE, "local", None),
        P(NODE, None, "local"),
        P(),
    )
    return jax.shard_map(
        on_device, mesh=fine, in_specs=in_specs, out_specs=out_specs, check_vma=False
    )
```

```python
import jax
import jax.numpy as jnp
from jax import lax
from jax.experimental import pallas as pl
from jax.experimental.pallas import tpu as pltpu
from jax.sharding import Mesh, PartitionSpec as P

BF16 = jnp.bfloat16
F32 = jnp.float32
NODE = ("chip", "core")


def copy_for_each(array, axis):
    copies = jnp.broadcast_to(array[None], (lax.axis_size(axis), *array.shape))
    return lax.all_to_all(copies, axis, 0, 0, tiled=True)


def activation_grads(gate_pre, up_pre, back_hidden, gate_col):
    logistic = jax.nn.sigmoid(gate_pre)
    swished = gate_pre * logistic
    hidden = swished * up_pre
    products = jnp.sum(hidden * back_hidden, axis=-1)
    scaled = gate_col * back_hidden
    grad_up = (scaled * swished).astype(BF16)
    grad_gate = (scaled * up_pre * logistic * (1.0 + gate_pre * (1.0 - logistic))).astype(BF16)
    weighted = (gate_col * hidden).astype(BF16)
    return weighted, grad_gate, grad_up, products


def slot_picks(named, capacity):
    count = named.shape[-1]
    earlier = jnp.arange(count)[:, None] < jnp.arange(count)[None, :]
    slot = jnp.einsum(
        "...s,st->...t", named.astype(BF16), earlier.astype(BF16), preferred_element_type=F32
    )
    slot = jnp.where(named, slot.astype(jnp.int32), -1)
    return (slot[..., None, :] == jnp.arange(capacity, dtype=jnp.int32)[:, None]).astype(BF16)


def ring_shift(array, ring, step):
    pairs = []
    for y in range(4):
        for z in range(4):
            target = ((y + step) % 4, z) if ring == "y" else (y, (z + step) % 4)
            pairs.append((4 * y + z, 4 * target[0] + target[1]))
    return lax.ppermute(array, "local", pairs)


def ring_gather(parts, rings):
    half = parts[0].shape[0] // 2
    count = range(len(parts))
    left = [ring_shift(parts[i], rings[i], 1) for i in count]
    right = [ring_shift(parts[i], rings[i], -1) for i in count]
    far_a = [ring_shift(left[i][:half], rings[i], 1) for i in count]
    far_b = [ring_shift(right[i][half:], rings[i], -1) for i in count]
    index = lax.axis_index("local")
    result = []
    for i in count:
        place = index // 4 if rings[i] == "y" else index % 4
        whole = jnp.zeros((4, *parts[i].shape), parts[i].dtype)
        across = jnp.concatenate([far_a[i], far_b[i]], axis=0)
        for value, step in ((parts[i], 0), (left[i], -1), (right[i], 1), (across, 2)):
            whole = lax.dynamic_update_index_in_dim(whole, value, (place + step) % 4, 0)
        result.append(whole)
    return result


def ring_scatter(parts, rings):
    half = parts[0].shape[1] // 2
    count = range(len(parts))
    index = lax.axis_index("local")
    place = [index // 4 if ring == "y" else index % 4 for ring in rings]

    def quarter(i, step):
        return lax.dynamic_index_in_dim(parts[i], (place[i] + step) % 4, 0, keepdims=False)

    across = [quarter(i, 2) for i in count]
    left = [ring_shift(across[i][:half], rings[i], 1) for i in count]
    right = [ring_shift(across[i][half:], rings[i], -1) for i in count]
    up = [quarter(i, 1) for i in count]
    up = [jnp.concatenate([up[i][:half] + left[i], up[i][half:]], axis=0) for i in count]
    down = [quarter(i, -1) for i in count]
    down = [jnp.concatenate([down[i][:half], down[i][half:] + right[i]], axis=0) for i in count]
    up = [ring_shift(up[i], rings[i], 1) for i in count]
    down = [ring_shift(down[i], rings[i], -1) for i in count]
    return [
        (quarter(i, 0).astype(F32) + up[i].astype(F32) + down[i].astype(F32)).astype(BF16)
        for i in count
    ]


def plane_scatter(low, high):
    kinds, rows, lanes = low.shape[2:]
    sums = [part.reshape(4, 4 * kinds, rows, lanes) for part in (low, high)]
    sums = ring_scatter(sums, ("y", "z"))
    sums = [part.reshape(4, 2 * kinds, rows // 2, lanes) for part in sums]
    sums = ring_scatter(sums, ("z", "y"))
    return [part.reshape(kinds, rows, lanes) for part in sums]


def plane_gather(part):
    rows, lanes = part.shape
    halves = [part[:, : lanes // 2], part[:, lanes // 2 :]]
    halves = [half.reshape(2, rows // 2, lanes // 2) for half in halves]
    halves = ring_gather(halves, ("z", "y"))
    halves = [half.reshape(4, rows, lanes // 2) for half in halves]
    return ring_gather(halves, ("y", "z"))


def cost(flops, size):
    return pl.CostEstimate(flops=flops, bytes_accessed=size, transcendentals=0)


def forward_body(tokens_ref, grads_ref, gate_ref, up_ref, down_ref, out_ref, low_ref, high_ref):
    quarters, _, rows, lanes = out_ref.shape
    part_lanes = low_ref.shape[-1]
    for kind, (left, right) in enumerate(
        ((tokens_ref, gate_ref), (tokens_ref, up_ref), (grads_ref, down_ref))
    ):
        slots = left[...].reshape(quarters * rows, left.shape[-1])
        part = jnp.dot(slots, right[0], preferred_element_type=F32).astype(BF16)
        part = part.reshape(quarters, rows, part.shape[-1])
        out_ref[:, kind] = part[..., :lanes]
        low_ref[0, :, kind] = part[..., lanes : lanes + part_lanes]
        high_ref[:, 0, kind] = part[..., lanes + part_lanes :]


def forward(token_rows, grad_rows, w_gate, w_up, w_down_t, quarters):
    nodes, own, capacity, width = token_rows.shape
    hidden = w_gate.shape[2]
    lanes = hidden // 4
    share = nodes * capacity // quarters
    rows = pl.BlockSpec((nodes, 1, capacity, width), lambda e: (0, e, 0, 0))
    weight = pl.BlockSpec((1, width, hidden), lambda e: (e, 0, 0))
    first = hidden - 2 * lanes
    return pl.pallas_call(
        forward_body,
        grid=(own,),
        in_specs=[rows, rows, weight, weight, weight],
        out_specs=[
            pl.BlockSpec((quarters, 3, share, first), lambda e: (e, 0, 0, 0)),
            pl.BlockSpec((1, quarters, 3, share, lanes), lambda e: (e, 0, 0, 0, 0)),
            pl.BlockSpec((quarters, 1, 3, share, lanes), lambda e: (0, e, 0, 0, 0)),
        ],
        out_shape=[
            jax.ShapeDtypeStruct((own * quarters, 3, share, first), BF16),
            jax.ShapeDtypeStruct((own, quarters, 3, share, lanes), BF16),
            jax.ShapeDtypeStruct((quarters, own, 3, share, lanes), BF16),
        ],
        name="forward",
        cost_estimate=cost(6 * own * nodes * capacity * width * hidden, 32 << 20),
    )(token_rows, grad_rows, w_gate, w_up, w_down_t)


def rows_body(grad_gate_ref, grad_up_ref, gate_ref, up_ref, cols_ref, out_ref):
    nodes, _, capacity, _ = out_ref.shape
    slots, extra = cols_ref.shape[1:]
    width = gate_ref.shape[1]
    hidden = gate_ref.shape[2]
    total = jnp.zeros((slots, width), F32)
    for left, right in ((grad_gate_ref, gate_ref), (grad_up_ref, up_ref)):
        total += lax.dot_general(
            left[...].reshape(slots, hidden),
            right[0],
            (((1,), (1,)), ((), ())),
            preferred_element_type=F32,
        )
    out_ref[:, 0, :, :width] = total.astype(BF16).reshape(nodes, capacity, width)
    out_ref[:, 0, :, width:] = cols_ref[0].reshape(nodes, capacity, extra)


def back_rows_of(first, w_gate, w_up, cols, nodes, quarters):
    own, width, hidden = w_gate.shape
    slots, extra = cols.shape[1:]
    share, capacity = slots // quarters, slots // nodes
    grads = [
        pl.BlockSpec((quarters, share, hidden), lambda e, kind=kind: (e, kind, 0))
        for kind in range(2)
    ]
    weight = pl.BlockSpec((1, width, hidden), lambda e: (e, 0, 0))
    return pl.pallas_call(
        rows_body,
        grid=(own,),
        in_specs=[*grads, weight, weight, pl.BlockSpec((1, slots, extra), lambda e: (e, 0, 0))],
        out_specs=pl.BlockSpec((nodes, 1, capacity, width + extra), lambda e: (0, e, 0, 0)),
        out_shape=jax.ShapeDtypeStruct((nodes, own, capacity, width + extra), BF16),
        name="back_rows",
        cost_estimate=cost(4 * own * slots * width * hidden, 20 << 20),
    )(first, first, w_gate, w_up, cols)


def weight_body(rows_ref, *refs):
    half = len(refs) // 2
    for grad_ref, out_ref in zip(refs[:half], refs[half:]):
        slots = rows_ref.shape[2]
        out_ref[0] = jnp.dot(
            rows_ref[0], grad_ref[...].reshape(slots, grad_ref.shape[-1]), preferred_element_type=F32
        ).astype(BF16)


def weight_grads(rows, grads, kinds, quarters):
    own, width, slots = rows.shape
    hidden = grads.shape[-1]
    share = slots // quarters
    out = pl.BlockSpec((1, width, hidden), lambda e: (e, 0, 0))
    return pl.pallas_call(
        weight_body,
        grid=(own,),
        in_specs=[pl.BlockSpec((1, width, slots), lambda e: (e, 0, 0))]
        + [
            pl.BlockSpec((quarters, share, hidden), lambda e, kind=kind: (e, kind, 0))
            for kind in range(kinds)
        ],
        out_specs=[out] * kinds,
        out_shape=[jax.ShapeDtypeStruct((own, width, hidden), BF16)] * kinds,
        name="weight_grads",
        cost_estimate=cost(2 * kinds * own * slots * width * hidden, 20 << 20),
    )(rows, *([grads] * kinds))


def down_body(rows_ref, low_ref, high_ref, out_ref):
    lanes = low_ref.shape[-1]
    slots = rows_ref.shape[2]
    for half, half_ref in enumerate((low_ref, high_ref)):
        out_ref[0, :, half * lanes : (half + 1) * lanes] = jnp.dot(
            rows_ref[0], half_ref[...].reshape(slots, lanes), preferred_element_type=F32
        ).astype(BF16)


def down_grads(rows, low, high):
    own, width, slots = rows.shape
    share, lanes = low.shape[2:]
    return pl.pallas_call(
        down_body,
        grid=(own,),
        in_specs=[
            pl.BlockSpec((1, width, slots), lambda e: (e, 0, 0)),
            pl.BlockSpec((1, 4, share, lanes), lambda e: (e, 0, 0, 0)),
            pl.BlockSpec((4, 1, share, lanes), lambda e: (0, e, 0, 0)),
        ],
        out_specs=pl.BlockSpec((1, width, 2 * lanes), lambda e: (e, 0, 0)),
        out_shape=jax.ShapeDtypeStruct((own, width, 2 * lanes), BF16),
        name="down_grads",
        cost_estimate=cost(4 * own * slots * width * lanes, 11 << 20),
    )(rows, low, high)


def on_device(tokens, grad_out, gates, routes, w_gate, w_up, w_down):
    nodes = lax.axis_size(NODE)
    me = lax.axis_index(NODE)
    tok_node, width = tokens.shape
    top_k = routes.shape[1]
    own = w_gate.shape[0]
    hidden = w_gate.shape[2]
    experts = own * nodes
    capacity = 5 * tok_node * top_k // (4 * experts)
    lanes = width + experts
    slots = nodes * capacity

    expert_ids = jnp.arange(experts, dtype=jnp.int32)
    choice = routes.T[:, None, :] == expert_ids[None, :, None]
    gate_of = jnp.sum(jnp.where(choice, gates.T[:, None, :].astype(F32), 0.0), axis=0).astype(BF16)
    packed = jnp.concatenate([tokens.T, gate_of], axis=0)
    all_tokens = lax.all_gather(packed, NODE, axis=0, tiled=False)
    first_core = lax.axis_index("core") == 0
    same = copy_for_each(grad_out.T, "chip")
    other = lax.ppermute(same, "core", [(0, 1), (1, 0)])
    all_grads = jnp.where(first_core, jnp.stack([same, other], 1), jnp.stack([other, same], 1))
    all_grads = all_grads.reshape(nodes, width, tok_node)

    all_gates = all_tokens[:, width : width + experts, :]
    loads = jnp.sum(all_gates.astype(F32), axis=(0, 2)) * (experts / (tok_node * top_k * 1.0))
    my_gates = lax.dynamic_slice_in_dim(all_tokens, width + me * own, own, axis=1)
    picks = slot_picks(my_gates > 0, capacity)
    gate_col = jnp.sum(picks.astype(F32) * my_gates[:, :, None, :].astype(F32), axis=-1)
    gate_col = jnp.swapaxes(gate_col, 0, 1).reshape(own, slots, 1)

    def rows_of(chosen, source):
        rows = jnp.einsum("bjct,bdt->bjcd", chosen, source, preferred_element_type=F32)
        return rows.astype(BF16)

    devices = lax.axis_size("local")
    place = lax.axis_index("local")
    quarters = devices // own
    share = slots // quarters
    token_rows = rows_of(picks, all_tokens[:, :width, :])
    grad_rows = rows_of(picks, all_grads)
    parts, low, high = forward(
        token_rows, grad_rows, w_gate, w_up, jnp.swapaxes(w_down, 1, 2), quarters
    )
    parts = parts.reshape(devices, 3 * share, parts.shape[-1])
    def columns_of(rows):
        return jnp.transpose(rows, (1, 3, 0, 2)).reshape(own, width, slots)

    token_columns, grad_columns = columns_of(token_rows), columns_of(grad_rows)
    sums = lax.psum_scatter(parts, "local", scatter_dimension=0, tiled=True)
    sums, token_columns, grad_columns = lax.optimization_barrier(
        (sums, token_columns, grad_columns)
    )
    sums = jnp.concatenate([sums.reshape(3, share, -1), *plane_scatter(low, high)], axis=-1)
    sums = sums.astype(F32)
    my_gate = lax.dynamic_slice_in_dim(gate_col.reshape(own * slots, 1), place * share, share)
    weighted, grad_gate, grad_up, products = activation_grads(sums[0], sums[1], sums[2], my_gate)
    first = jnp.concatenate([grad_gate, grad_up], axis=0)
    first = lax.all_gather(first, "local", axis=0, tiled=False)
    grad_wd = jnp.swapaxes(down_grads(grad_columns, *plane_gather(weighted)), 1, 2)
    products = copy_for_each(products.astype(BF16)[None], "local").reshape(own, slots)
    expert_of = me * own + jnp.arange(own, dtype=jnp.int32)
    marks = expert_of[:, None, None] == expert_ids
    cols = jnp.where(marks, products[..., None], jnp.zeros((), BF16))
    first, grad_wd = lax.optimization_barrier((first, grad_wd))
    back_rows = back_rows_of(first, w_gate, w_up, cols, nodes, quarters)
    core = lax.axis_index("core")
    picks_by_core = picks.reshape(nodes // 2, 2, own, capacity, tok_node)
    rows_by_core = back_rows.reshape(nodes // 2, 2, own, capacity, lanes)

    def sums_for(which):
        return jnp.einsum(
            "bjct,bjcd->bdt",
            lax.dynamic_index_in_dim(picks_by_core, which, 1, keepdims=False),
            lax.dynamic_index_in_dim(rows_by_core, which, 1, keepdims=False),
            preferred_element_type=F32,
        ).astype(BF16)

    taken = lax.ppermute(sums_for(1 - core), "core", [(0, 1), (1, 0)])
    kept = sums_for(core)
    token_sums = (kept.astype(F32) + taken.astype(F32)).astype(BF16)
    token_sums = lax.all_to_all(token_sums, "chip", 0, 0, tiled=True)
    home = jnp.sum(token_sums.astype(F32), axis=0)

    grad_wg, grad_wu = weight_grads(token_columns, first, 2, quarters)
    grad_tokens = home[:width].astype(BF16).T
    products_home = home[width : width + experts]
    grad_gates = jnp.sum(jnp.where(choice, products_home[None], 0.0), axis=1).astype(BF16).T
    return (grad_tokens, grad_gates, grad_wg, grad_wu, grad_wd, loads)


def solution(mesh):
    nodes, devices = mesh.shape["node"], mesh.shape["local"]
    fine = Mesh(mesh.devices.reshape(nodes // 2, 2, devices), ("chip", "core", "local"))
    in_specs = (
        P(NODE, "local"),
        P(NODE, "local"),
        P(NODE, None),
        P(NODE, None),
        P(NODE, "local", None),
        P(NODE, "local", None),
        P(NODE, None, "local"),
    )
    out_specs = (
        P(NODE, "local"),
        P(NODE, None),
        P(NODE, "local", None),
        P(NODE, "local", None),
        P(NODE, None, "local"),
        P(),
    )
    return jax.shard_map(
        on_device, mesh=fine, in_specs=in_specs, out_specs=out_specs, check_vma=False
    )
```
